256 devices in a mesh: gx: 32 (over z, y_hi, core), gy: 8 (over y_lo, x).
Axes of the slice: x: 4, y: 4 (y_hi: 2, y_lo: 2; y = y_hi * 2 + y_lo), z: 8, core: 2. Of those that a mesh axis runs over, the one named last changes fastest.
Arguments:
- prognostic_values: float32 [3, 6, 4096, 4096], P(None, None, 'gx', 'gy'), may hold values from -6 to 6
- forcing_host_values: bfloat16 [3, 6, 4096, 4096], P(None, None, 'gx', 'gy'), may hold values from -6 to 6
- strength: float32 [3, 6], replicated, may hold values from 50 to 200
- level_height: float32 [3], replicated, may hold values from 0.2 to 3
- pbl_height: float32 [4096, 4096], P('gx', 'gy'), may hold values from 0.2 to 3
Outputs:
- tendency: bfloat16 [3, 6, 4096, 4096], P(None, None, 'gx', 'gy')
- energy: float32 [3, 6], replicated
The draws below stay inside these ranges and needn't reach their ends.
All inputs are finite; a program needn't handle non-finite values.
Results may differ from the reference program's by a relative error of at most 0.001.
Values sent between devices are 32-bit elements; how exact they have to be, the bound alone decides.
No kernel may reach another device: no remote copies, remote signals or barrier semaphores. Data moves between devices by JAX's collectives and lax.ppermute only.
A program may use at most 64 MiB of HBM per device.

```python
import math
import jax
import jax.numpy as jnp
from jax import lax

KX = 32
KY = 32
VARS = 6
LEV = 3
NX = 4096
NY = 4096


def level_of(rng, extent, cuts, low, high):
    def one(dim, shards_of):
        steps = jax.random.uniform(jax.random.fold_in(jax.random.fold_in(rng, 6), dim), (shards_of,), jnp.float32, low / len(cuts), high / len(cuts))
        return jnp.repeat(jnp.exp(steps), extent[dim] // shards_of).reshape((-1,) + (1,) * (len(extent) - dim - 1))

    gain = one(*cuts[0])
    for cut in cuts[1:]:
        gain = gain * one(*cut)
    return gain


def gaussian(own_key, extent, deviation, most, shards=(), dtype=jnp.bfloat16):
    level = level_of(own_key, extent, shards, -0.22, 0.18) if shards else 1.0
    values = jax.random.normal(own_key, extent, jnp.float32) * deviation * level
    return jnp.minimum(jnp.maximum(values, -most), most).astype(dtype)


def setup_inputs(seed: int = 0) -> dict:
    seeds = jax.random.split(jax.random.key(seed), 6)
    prognostic_values = gaussian(seeds[0], (LEV, VARS, NX, NY), 1.0, 6.0, ((2, 32), (3, 8)), jnp.float32)
    forcing_host_values = gaussian(seeds[1], (LEV, VARS, NX, NY), 1.0, 6.0, ((2, 32), (3, 8)))
    strength = jnp.clip(jnp.exp(jax.random.uniform(seeds[2], (LEV, VARS), jnp.float32, math.log(50.0), math.log(200.0))), 50.0, 200.0)
    level_height = jnp.clip(jax.random.uniform(seeds[3], (LEV,), jnp.float32, 0.2, 3.0), 0.2, 3.0)
    pbl_height = jnp.clip(0.2 + 2.8 * jax.random.uniform(seeds[4], (NX, NY), jnp.float32) ** level_of(seeds[4], (NX, NY), ((0, 32), (1, 8)), -0.2, 0.2), 0.2, 3.0)
    return {"prognostic_values": prognostic_values, "forcing_host_values": forcing_host_values, "strength": strength, "level_height": level_height, "pbl_height": pbl_height}


ramp_depth = 0.25

def cosine_table(total, modes, start, count):
    index = (start + jnp.arange(count)).astype(jnp.float32)
    waves = jnp.arange(modes).astype(jnp.float32)
    scales = jnp.where(waves == 0.0, jnp.sqrt(1.0 / total), jnp.sqrt(2.0 / total)).astype(jnp.float32)
    return scales[None, :] * jnp.cos(jnp.pi * (index[:, None] + 0.5) * waves[None, :] / total)

def reference(prognostic_values, forcing_host_values, strength, level_height, pbl_height):
    meridional_cosines = cosine_table(NX, KX, 0, NX)
    col_basis = cosine_table(NY, KY, 0, NY)
    largest_wavenumber = lax.Precision.HIGHEST

    def one_level(items):
        model, driver, gains, altitude_factor = items
        diff = driver.astype(jnp.float32) - model
        part = jnp.einsum('vij,jb->vib', diff, col_basis, precision=largest_wavenumber)
        mode_factors = jnp.einsum('wl,ywg->ylg', meridional_cosines, part, precision=largest_wavenumber)
        restored_fields = jnp.einsum('ky,jyp->jkp', meridional_cosines, mode_factors, precision=largest_wavenumber)
        recon = jnp.einsum('vib,jb->vij', restored_fields, col_basis, precision=largest_wavenumber)
        damping_share = 1.0 / (1.0 + jnp.exp(-(altitude_factor - pbl_height) / ramp_depth))
        tend = (gains[:, None, None] * damping_share[None] * recon).astype(jnp.bfloat16)
        energy = lax.optimization_barrier(jnp.sum(recon * recon, axis=(1, 2))) / (KX * KY)
        return (tend, energy)
    tendency, energy = lax.map(one_level, (prognostic_values, forcing_host_values, strength, level_height))
    return (tendency, energy)
```

```python
import math

import jax
import jax.numpy as jnp
from jax import lax
from jax.experimental import pallas as pl
from jax.experimental.pallas import tpu as pltpu
from jax.sharding import PartitionSpec as P

MODES = 32
RAMP = 0.25
BOTH = ("gx", "gy")
F32, BF16 = jnp.float32, jnp.bfloat16


def position(x, y, z, core):
    return ((z * 4 + (y // 2) * 2 + core) * 8) + (y % 2) * 4 + x


def grouped(key, order):
    found = {}
    for z in range(8):
        for y in range(4):
            for x in range(4):
                for core in range(2):
                    place = (x, y, z, core)
                    found.setdefault(key(*place), []).append((order(*place), position(*place)))
    return [[at for _, at in sorted(group)] for _, group in sorted(found.items())]


SHARE = (0, 1, 1, 0)
NEAR = grouped(lambda x, y, z, c: (y // 2, z), lambda x, y, z, c: (SHARE[y], x, c))
FAR = grouped(lambda x, y, z, c: (x, SHARE[y], c), lambda x, y, z, c: (z, y))
SHARES = 16


def cosines(index, wave, total):
    turn = ((2 * index + 1) * wave) & (4 * total - 1)
    turn = jnp.where(turn > 2 * total, 4 * total - turn, turn)
    y = (total - turn).astype(F32) * F32(math.pi / (2 * total))
    square = y * y
    series = F32(1.0 / math.factorial(13))
    for power in (11, 9, 7, 5, 3, 1):
        sign = -1.0 if power % 4 == 3 else 1.0
        series = series * square + F32(sign / math.factorial(power))
    scale = jnp.where(wave == 0, F32(math.sqrt(1.0 / total)), F32(math.sqrt(2.0 / total)))
    return scale * (y * series)


def split(value):
    high = value.astype(BF16)
    return high, (value - high.astype(F32)).astype(BF16)


def iota(shape, dim):
    return lax.broadcasted_iota(jnp.int32, shape, dim)


def dot(a, b):
    return jnp.dot(a, b, preferred_element_type=F32)


def analysis(levels, variables, nx, ny, p_hbm, f_hbm, out_ref, p_buf, f_buf, p_sem, f_sem, w_ref):
    rows, cols = p_hbm.shape[2], p_hbm.shape[3]
    fields = [(l, v) for l in range(levels) for v in range(variables)]
    copies = []
    for k, (l, v) in enumerate(fields):
        pair = (
            pltpu.make_async_copy(p_hbm.at[l, v], p_buf.at[k], p_sem.at[k]),
            pltpu.make_async_copy(f_hbm.at[l, v], f_buf.at[k], f_sem.at[k]),
        )
        for copy in pair:
            copy.start()
        copies.append(pair)

    row0 = lax.axis_index("gx") * rows
    col0 = lax.axis_index("gy") * cols
    wide = 4 * MODES
    table = cosines(col0 + iota((cols, wide), 0), iota((cols, wide), 1) & (MODES - 1), ny)
    high, low = split(table)
    w_ref[:, :wide] = high
    w_ref[:, wide:] = low
    table = cosines(row0 + iota((MODES, rows), 1), iota((MODES, rows), 0), nx)
    row_table = jnp.concatenate(split(table), axis=0)
    lane_group = iota((8, wide), 1) // MODES

    for k in range(len(fields)):
        for copy in copies[k]:
            copy.wait()
        diff_high, diff_low = split(f_buf[k].astype(F32) - p_buf[k])
        both = dot(diff_high, w_ref[...]) + dot(diff_low, w_ref[...])
        part_high, part_low = split(both[:, :wide] + both[:, wide:])
        both = dot(row_table, part_high) + dot(row_table, part_low)
        coefs = both[:MODES] + both[MODES:]
        tile = coefs[:8]
        for q in range(1, 4):
            tile = jnp.where(lane_group == q, coefs[8 * q : 8 * q + 8], tile)
        out_ref[8 * k : 8 * k + 8, :] = tile


def synthesis(
    levels, variables, nx, ny,
    strength_ref, level_ref, c_ref, pbl_ref, out_hbm, energy_ref, o_buf, weight_ref, o_sem, t_ref,
):
    rows, cols = pbl_ref.shape
    row0 = lax.axis_index("gx") * rows
    col0 = lax.axis_index("gy") * cols
    wide = 4 * MODES
    for l in range(levels):
        weight_ref[l] = 1.0 / (1.0 + jnp.exp(-(level_ref[l] - pbl_ref[...]) / F32(RAMP)))
    lane_group = iota((1, wide), 1) // MODES
    high, low = split(cosines(row0 + iota((rows, wide), 0), iota((rows, wide), 1) & (MODES - 1), nx))
    none = jnp.zeros_like(high)
    row_table = jnp.where(lane_group < 2, high, jnp.where(lane_group == 2, low, none))
    high, low = split(cosines(col0 + iota((MODES, cols), 1), iota((MODES, cols), 0), ny))
    t_ref[0:32, :] = high
    t_ref[32:64, :] = high
    t_ref[64:96, :] = low
    t_ref[96:128, :] = jnp.zeros_like(high)

    at = (iota((levels, variables), 0), iota((levels, variables), 1))
    energy = jnp.zeros((levels, variables), F32)
    copies = []
    for l in range(levels):
        for v in range(variables):
            k = l * variables + v
            tile = c_ref[8 * k : 8 * k + 8, :]
            total = jnp.sum(tile * tile) / F32(MODES * MODES)
            energy = jnp.where((at[0] == l) & (at[1] == v), total, energy)
            tile = tile * strength_ref[l, v]
            blocks = []
            for q in range(4):
                one = jnp.where(lane_group == q, tile, 0.0)
                one = one + pltpu.roll(one, MODES, 1)
                blocks.append(one + pltpu.roll(one, 2 * MODES, 1))
            high, low = split(jnp.concatenate(blocks, axis=0))
            coefs = jnp.concatenate([high, low, high, jnp.zeros_like(high)], axis=0)
            high, low = split(dot(row_table, coefs))
            restored = jnp.where(lane_group == 1, low, high)
            recon = dot(restored, t_ref[...])
            o_buf[k] = (weight_ref[l] * recon).astype(BF16)
            copy = pltpu.make_async_copy(o_buf.at[k], out_hbm.at[l, v], o_sem.at[k])
            copy.start()
            copies.append(copy)
    energy_ref[...] = energy
    for copy in copies:
        copy.wait()


def per_device(prognostic_values, forcing_host_values, strength, level_height, pbl_height):
    levels, variables, rows, cols = prognostic_values.shape
    nx, ny = rows * lax.axis_size("gx"), cols * lax.axis_size("gy")
    count = levels * variables
    lines = 8 * count
    shapes = (levels, variables, nx, ny)
    anywhere = pl.BlockSpec(memory_space=pl.ANY)
    vmem = pl.BlockSpec(memory_space=pltpu.VMEM)
    smem = pl.BlockSpec(memory_space=pltpu.SMEM)

    mine = pl.pallas_call(
        lambda *refs: analysis(*shapes, *refs),
        name="analysis",
        out_shape=jax.ShapeDtypeStruct((lines, 128), F32),
        in_specs=[anywhere, anywhere],
        out_specs=vmem,
        scratch_shapes=[
            pltpu.VMEM((count, rows, cols), F32),
            pltpu.VMEM((count, rows, cols), BF16),
            pltpu.SemaphoreType.DMA((count,)),
            pltpu.SemaphoreType.DMA((count,)),
            pltpu.VMEM((cols, 8 * MODES), BF16),
        ],
    )(prognostic_values, forcing_host_values)

    length = lines * 128 // SHARES
    shares = mine.reshape(SHARES, 1, length)
    got = lax.all_to_all(shares, BOTH, 0, 0, tiled=True, axis_index_groups=NEAR)
    share = jnp.broadcast_to(jnp.sum(got, axis=0, keepdims=True), (SHARES, 1, length))
    got = lax.all_to_all(share, BOTH, 0, 0, tiled=True, axis_index_groups=FAR)
    share = jnp.broadcast_to(jnp.sum(got, axis=0, keepdims=True), (SHARES, 1, length))
    coefs = lax.all_to_all(share, BOTH, 0, 0, tiled=True, axis_index_groups=NEAR)
    coefs = coefs.reshape(lines, 128)

    tendency, energy = pl.pallas_call(
        lambda *refs: synthesis(*shapes, *refs),
        name="synthesis",
        out_shape=(
            jax.ShapeDtypeStruct((levels, variables, rows, cols), BF16),
            jax.ShapeDtypeStruct((levels, variables), F32),
        ),
        in_specs=[smem, smem, vmem, vmem],
        out_specs=(anywhere, vmem),
        scratch_shapes=[
            pltpu.VMEM((count, rows, cols), BF16),
            pltpu.VMEM((levels, rows, cols), F32),
            pltpu.SemaphoreType.DMA((count,)),
            pltpu.VMEM((4 * MODES, cols), BF16),
        ],
    )(strength, level_height, coefs, pbl_height)
    return tendency, energy


def solution(mesh):
    return jax.shard_map(
        per_device,
        mesh=mesh,
        in_specs=(P(None, None, "gx", "gy"), P(None, None, "gx", "gy"), P(), P(), P("gx", "gy")),
        out_specs=(P(None, None, "gx", "gy"), P()),
        check_vma=False,
    )
```

```python
import math

import jax
import jax.numpy as jnp
from jax import lax
from jax.experimental import pallas as pl
from jax.experimental.pallas import tpu as pltpu
from jax.sharding import PartitionSpec as P

MODES = 32
RAMP = 0.25
BOTH = ("gx", "gy")
F32, BF16 = jnp.float32, jnp.bfloat16


def position(x, y, z, core):
    return ((z * 4 + (y // 2) * 2 + core) * 8) + (y % 2) * 4 + x


def partners(move):
    places = [(x, y, z, c) for z in range(8) for y in range(4) for x in range(4) for c in range(2)]
    return [(position(*place), position(*move(*place))) for place in places]


CHIP = partners(lambda x, y, z, c: (x, y, z, 1 - c))
EXCHANGES = (
    (
        partners(lambda x, y, z, c: (x ^ 1, y, z, 1 - c)),
        partners(lambda x, y, z, c: (x ^ 2, y, z, c)),
        partners(lambda x, y, z, c: (x ^ 3, y, z, 1 - c)),
    ),
    (
        partners(lambda x, y, z, c: (x, y ^ 1, z, 1 - c)),
        partners(lambda x, y, z, c: (x, y ^ 2, z, c)),
        partners(lambda x, y, z, c: (x, y ^ 3, z, 1 - c)),
    ),
    (partners(lambda x, y, z, c: (x, y, z ^ 1, 1 - c)),),
    (partners(lambda x, y, z, c: (x, y, z ^ 3, 1 - c)),),
    (partners(lambda x, y, z, c: (x, y, z ^ 7, 1 - c)),),
)


def half_held():
    gx, gy = lax.axis_index("gx"), lax.axis_index("gy")
    return (gx // 4 + gx + gy // 4 + gy) & 1


def cosines(index, wave, total):
    turn = ((2 * index + 1) * wave) & (4 * total - 1)
    turn = jnp.where(turn > 2 * total, 4 * total - turn, turn)
    y = (total - turn).astype(F32) * F32(math.pi / (2 * total))
    square = y * y
    series = F32(1.0 / math.factorial(13))
    for power in (11, 9, 7, 5, 3, 1):
        sign = -1.0 if power % 4 == 3 else 1.0
        series = series * square + F32(sign / math.factorial(power))
    scale = jnp.where(wave == 0, F32(math.sqrt(1.0 / total)), F32(math.sqrt(2.0 / total)))
    return scale * (y * series)


def split(value):
    high = value.astype(BF16)
    return high, (value - high.astype(F32)).astype(BF16)


def iota(shape, dim):
    return lax.broadcasted_iota(jnp.int32, shape, dim)


def dot(a, b):
    return jnp.dot(a, b, preferred_element_type=F32)


CHUNK = 6


def analysis(
    levels, variables, nx, ny, p_hbm, f_hbm, mine_ref, other_ref, p_buf, f_buf, p_sem, f_sem, w_ref, out_ref
):
    rows, cols = p_hbm.shape[2], p_hbm.shape[3]
    fields = [(l, v) for l in range(levels) for v in range(variables)]
    copies = []
    for k, (l, v) in enumerate(fields):
        pair = (
            pltpu.make_async_copy(p_hbm.at[l, v], p_buf.at[k], p_sem.at[k]),
            pltpu.make_async_copy(f_hbm.at[l, v], f_buf.at[k], f_sem.at[k]),
        )
        for copy in pair:
            copy.start()
        copies.append(pair)

    row0 = lax.axis_index("gx") * rows
    col0 = lax.axis_index("gy") * cols
    wide = 4 * MODES
    table = cosines(col0 + iota((cols, wide), 0), iota((cols, wide), 1) & (MODES - 1), ny)
    high, low = split(table)
    w_ref[:, :wide] = high
    w_ref[:, wide:] = low
    table = cosines(row0 + iota((MODES, rows), 1), iota((MODES, rows), 0), nx)
    high, low = split(table)
    row_table = jnp.concatenate(
        [jnp.concatenate([high, high], axis=1), jnp.concatenate([low, low], axis=1)], axis=0
    )
    lane_group = iota((8, wide), 1) // MODES

    for start in range(0, len(fields), CHUNK):
        chunk = range(start, min(start + CHUNK, len(fields)))
        for k in chunk:
            for copy in copies[k]:
                copy.wait()
        highs, lows = zip(*(split(f_buf[k].astype(F32) - p_buf[k]) for k in chunk))
        both = dot(jnp.concatenate(highs + lows, axis=0), w_ref[...])
        both = both[: len(chunk) * rows] + both[len(chunk) * rows :]
        high, low = split(both[:, :wide] + both[:, wide:])
        high = [high[i * rows : (i + 1) * rows] for i in range(len(chunk))]
        low = [low[i * rows : (i + 1) * rows] for i in range(len(chunk))]
        for i in range(0, len(chunk), 2):
            parts = [jnp.concatenate(part[i : i + 2], axis=1) for part in (high, low)]
            both = dot(row_table, jnp.concatenate(parts, axis=0))
            coefs = both[:MODES] + both[MODES:]
            for j, k in enumerate(chunk[i : i + 2]):
                tile = coefs[:8, wide * j : wide * (j + 1)]
                for q in range(1, 4):
                    part = coefs[8 * q : 8 * q + 8, wide * j : wide * (j + 1)]
                    tile = jnp.where(lane_group == q, part, tile)
                out_ref[8 * k : 8 * k + 8, :] = tile
    half = out_ref.shape[0] // 2
    first, second = out_ref[:half, :], out_ref[half:, :]
    held = half_held() == 0
    mine_ref[...] = jnp.where(held, first, second)
    other_ref[...] = jnp.where(held, second, first)


def preparation(levels, nx, ny, level_ref, pbl_ref, weight_ref, r_ref, t_ref):
    rows, cols = pbl_ref.shape
    row0 = lax.axis_index("gx") * rows
    col0 = lax.axis_index("gy") * cols
    wide = 4 * MODES
    for l in range(levels):
        weight_ref[l] = 1.0 / (1.0 + jnp.exp(-(level_ref[l] - pbl_ref[...]) / F32(RAMP)))
    lane_group = iota((1, wide), 1) // MODES
    high, low = split(cosines(row0 + iota((rows, wide), 0), iota((rows, wide), 1) & (MODES - 1), nx))
    none = jnp.zeros_like(high)
    r_ref[...] = jnp.where(lane_group < 2, high, jnp.where(lane_group == 2, low, none))
    high, low = split(cosines(col0 + iota((MODES, cols), 1), iota((MODES, cols), 0), ny))
    t_ref[0:32, :] = high
    t_ref[32:64, :] = high
    t_ref[64:96, :] = low
    t_ref[96:128, :] = jnp.zeros_like(high)


def synthesis(
    levels, variables,
    strength_ref, mine_ref, other_ref, weight_ref, r_ref, t_ref, out_hbm, energy_ref, o_buf, o_sem, z_ref,
):
    wide = 4 * MODES
    lane_group = iota((1, wide), 1) // MODES
    held = half_held() == 0
    half = levels * variables // 2
    at = (iota((levels, variables), 0), iota((levels, variables), 1))
    energy = jnp.zeros((levels, variables), F32)
    fields = [(l, v) for l in range(levels) for v in range(variables)]
    for start in range(0, len(fields), 2):
        sides = []
        for k in (start, start + 1):
            l, v = fields[k]
            line = 8 * (k % half)
            ours, theirs = mine_ref[line : line + 8, :], other_ref[line : line + 8, :]
            tile = jnp.where(held, ours, theirs) if k < half else jnp.where(held, theirs, ours)
            total = jnp.sum(tile * tile) / F32(MODES * MODES)
            energy = jnp.where((at[0] == l) & (at[1] == v), total, energy)
            tile = tile * strength_ref[l, v]
            blocks = []
            for q in range(4):
                one = jnp.where(lane_group == q, tile, 0.0)
                one = one + pltpu.roll(one, MODES, 1)
                blocks.append(one + pltpu.roll(one, 2 * MODES, 1))
            high, low = split(jnp.concatenate(blocks, axis=0))
            sides.append(jnp.concatenate([high, low, high, jnp.zeros_like(high)], axis=0))
        both = dot(r_ref[...], jnp.concatenate(sides, axis=1))
        for i, k in enumerate((start, start + 1)):
            high, low = split(both[:, wide * i : wide * (i + 1)])
            z_ref[k] = jnp.where(lane_group == 1, low, high)
    energy_ref[...] = energy

    copies = []
    for k, (l, v) in enumerate(fields):
        o_buf[k] = (weight_ref[l] * dot(z_ref[k], t_ref[...])).astype(BF16)
        copies.append(pltpu.make_async_copy(o_buf.at[k], out_hbm.at[l, v], o_sem.at[k]))
        if k:
            copies[k - 1].start()
    copies[-1].start()
    for copy in copies:
        copy.wait()


def in_vmem(value):
    return pltpu.with_memory_space_constraint(value, pltpu.VMEM)


def per_device(prognostic_values, forcing_host_values, strength, level_height, pbl_height):
    levels, variables, rows, cols = prognostic_values.shape
    nx, ny = rows * lax.axis_size("gx"), cols * lax.axis_size("gy")
    count = levels * variables
    lines = 8 * count
    wide = 4 * MODES
    anywhere = pl.BlockSpec(memory_space=pl.ANY)
    vmem = pl.BlockSpec(memory_space=pltpu.VMEM)
    smem = pl.BlockSpec(memory_space=pltpu.SMEM)

    mine, other = pl.pallas_call(
        lambda *refs: analysis(levels, variables, nx, ny, *refs),
        name="analysis",
        out_shape=(pltpu.VMEM((lines // 2, wide), F32), pltpu.VMEM((lines // 2, wide), F32)),
        in_specs=[anywhere, anywhere],
        out_specs=(vmem, vmem),
        scratch_shapes=[
            pltpu.VMEM((count, rows, cols), F32),
            pltpu.VMEM((count, rows, cols), BF16),
            pltpu.SemaphoreType.DMA((count,)),
            pltpu.SemaphoreType.DMA((count,)),
            pltpu.VMEM((cols, 2 * wide), BF16),
            pltpu.VMEM((lines, wide), F32),
        ],
    )(prognostic_values, forcing_host_values)

    weight, row_table, col_table = pl.pallas_call(
        lambda *refs: preparation(levels, nx, ny, *refs),
        name="preparation",
        out_shape=(
            pltpu.VMEM((levels, rows, cols), F32),
            pltpu.VMEM((rows, wide), BF16),
            pltpu.VMEM((wide, cols), BF16),
        ),
        in_specs=[smem, vmem],
        out_specs=(vmem, vmem, vmem),
    )(level_height, in_vmem(pbl_height))

    held = mine + lax.ppermute(other, BOTH, CHIP)
    prepared = (weight, row_table, col_table)
    for at, exchange in enumerate(EXCHANGES):
        if at == len(EXCHANGES) - 1:
            held, prepared = lax.optimization_barrier((held, prepared))
        held = sum((lax.ppermute(held, BOTH, pairs) for pairs in exchange), held)
    other = lax.ppermute(held, BOTH, CHIP)

    tendency, energy = pl.pallas_call(
        lambda *refs: synthesis(levels, variables, *refs),
        name="synthesis",
        out_shape=(
            jax.ShapeDtypeStruct((levels, variables, rows, cols), BF16),
            jax.ShapeDtypeStruct((levels, variables), F32),
        ),
        in_specs=[smem, vmem, vmem, vmem, vmem, vmem],
        out_specs=(anywhere, vmem),
        scratch_shapes=[
            pltpu.VMEM((count, rows, cols), BF16),
            pltpu.SemaphoreType.DMA((count,)),
            pltpu.VMEM((count, rows, wide), BF16),
        ],
    )(strength, in_vmem(held), in_vmem(other), *map(in_vmem, prepared))
    return tendency, energy


def solution(mesh):
    return jax.shard_map(
        per_device,
        mesh=mesh,
        in_specs=(P(None, None, "gx", "gy"), P(None, None, "gx", "gy"), P(), P(), P("gx", "gy")),
        out_specs=(P(None, None, "gx", "gy"), P()),
        check_vma=False,
    )
```

```python
import math

import jax
import jax.numpy as jnp
from jax import lax
from jax.experimental import pallas as pl
from jax.experimental.pallas import tpu as pltpu
from jax.sharding import PartitionSpec as P

MODES = 32
RAMP = 0.25
BOTH = ("gx", "gy")
F32, BF16 = jnp.float32, jnp.bfloat16


def position(x, y, z, core):
    return ((z * 4 + (y // 2) * 2 + core) * 8) + (y % 2) * 4 + x


def partners(move):
    places = [(x, y, z, c) for z in range(8) for y in range(4) for x in range(4) for c in range(2)]
    return [(position(*place), position(*move(*place))) for place in places]


CHIP = partners(lambda x, y, z, c: (x, y, z, 1 - c))
EXCHANGES = (
    (
        partners(lambda x, y, z, c: (x ^ 1, y, z, 1 - c)),
        partners(lambda x, y, z, c: (x ^ 2, y, z, c)),
        partners(lambda x, y, z, c: (x ^ 3, y, z, 1 - c)),
    ),
    (
        partners(lambda x, y, z, c: (x, y ^ 1, z, 1 - c)),
        partners(lambda x, y, z, c: (x, y ^ 2, z, c)),
        partners(lambda x, y, z, c: (x, y ^ 3, z, 1 - c)),
    ),
    (partners(lambda x, y, z, c: (x, y, z ^ 1, 1 - c)),),
    (partners(lambda x, y, z, c: (x, y, z ^ 3, 1 - c)),),
    (partners(lambda x, y, z, c: (x, y, z ^ 7, 1 - c)),),
)


def half_held():
    gx, gy = lax.axis_index("gx"), lax.axis_index("gy")
    return (gx // 4 + gx + gy // 4 + gy) & 1


def cosines(index, wave, total):
    turn = ((2 * index + 1) * wave) & (4 * total - 1)
    turn = jnp.where(turn > 2 * total, 4 * total - turn, turn)
    y = (total - turn).astype(F32) * F32(math.pi / (2 * total))
    square = y * y
    series = F32(1.0 / math.factorial(13))
    for power in (11, 9, 7, 5, 3, 1):
        sign = -1.0 if power % 4 == 3 else 1.0
        series = series * square + F32(sign / math.factorial(power))
    scale = jnp.where(wave == 0, F32(math.sqrt(1.0 / total)), F32(math.sqrt(2.0 / total)))
    return scale * (y * series)


def split(value):
    high = value.astype(BF16)
    return high, (value - high.astype(F32)).astype(BF16)


def iota(shape, dim):
    return lax.broadcasted_iota(jnp.int32, shape, dim)


def dot(a, b):
    return jnp.dot(a, b, preferred_element_type=F32)


CHUNK = 6


def analysis(
    count, nx, ny, p_hbm, f_hbm, mine_ref, other_ref, p_buf, f_buf, p_sem, f_sem, w_ref, out_ref
):
    rows, cols = p_hbm.shape[1:]
    copies = []
    for at, start in enumerate(range(0, count, CHUNK)):
        chunk = pl.ds(start, CHUNK)
        pair = (
            pltpu.make_async_copy(p_hbm.at[chunk], p_buf.at[chunk], p_sem.at[at]),
            pltpu.make_async_copy(f_hbm.at[chunk], f_buf.at[chunk], f_sem.at[at]),
        )
        for copy in pair:
            copy.start()
        copies.append(pair)

    row0 = lax.axis_index("gx") * rows
    col0 = lax.axis_index("gy") * cols
    wide = 4 * MODES
    table = cosines(col0 + iota((cols, wide), 0), iota((cols, wide), 1) & (MODES - 1), ny)
    high, low = split(table)
    w_ref[:, :wide] = high
    w_ref[:, wide:] = low
    table = cosines(row0 + iota((MODES, rows), 1), iota((MODES, rows), 0), nx)
    high, low = split(table)
    row_table = jnp.concatenate(
        [jnp.concatenate([high, high], axis=1), jnp.concatenate([low, low], axis=1)], axis=0
    )
    lane_group = iota((8, wide), 1) // MODES

    for pair, start in zip(copies, range(0, count, CHUNK)):
        for copy in pair:
            copy.wait()
        parts = []
        for k in range(start, start + CHUNK):
            diff = jnp.concatenate(split(f_buf[k].astype(F32) - p_buf[k]), axis=0)
            both = dot(row_table, diff)
            parts.append(both[:MODES] + both[MODES:])
        part = jnp.concatenate(split(jnp.concatenate(parts, axis=0)), axis=0)
        both = dot(part, w_ref[...])
        both = both[: CHUNK * MODES] + both[CHUNK * MODES :]
        both = both[:, :wide] + both[:, wide:]
        for i in range(CHUNK):
            coefs = both[MODES * i : MODES * (i + 1)]
            tile = coefs[:8]
            for q in range(1, 4):
                tile = jnp.where(lane_group == q, coefs[8 * q : 8 * q + 8], tile)
            line = 8 * (start + i)
            out_ref[line : line + 8, :] = tile
    half = out_ref.shape[0] // 2
    first, second = out_ref[:half, :], out_ref[half:, :]
    held = half_held() == 0
    mine_ref[...] = jnp.where(held, first, second)
    other_ref[...] = jnp.where(held, second, first)


def preparation(
    levels, variables, nx, ny, strength_ref, level_ref, pbl_ref, weight_ref, r_ref, t_ref, scale_ref
):
    rows, cols = pbl_ref.shape
    row0 = lax.axis_index("gx") * rows
    col0 = lax.axis_index("gy") * cols
    wide = 4 * MODES
    for l in range(levels):
        weight_ref[l] = 1.0 / (1.0 + jnp.exp(-(level_ref[l] - pbl_ref[...]) / F32(RAMP)))
        for v in range(variables):
            scale_ref[l * variables + v] = jnp.full((8, wide), strength_ref[l, v], F32)
    lane_group = iota((1, wide), 1) // MODES
    high, low = split(cosines(row0 + iota((rows, wide), 0), iota((rows, wide), 1) & (MODES - 1), nx))
    none = jnp.zeros_like(high)
    r_ref[...] = jnp.where(lane_group < 2, high, jnp.where(lane_group == 2, low, none))
    high, low = split(cosines(col0 + iota((MODES, cols), 1), iota((MODES, cols), 0), ny))
    t_ref[0:32, :] = high
    t_ref[32:64, :] = high
    t_ref[64:96, :] = low
    t_ref[96:128, :] = jnp.zeros_like(high)


AHEAD = 6


def synthesis(
    levels, variables,
    mine_ref, other_ref, weight_ref, r_ref, t_ref, scale_ref,
    out_hbm, energy_hbm, o_buf, o_sem, z_ref, e_ref, e_sem,
):
    count = levels * variables
    wide = 4 * MODES
    lane_group = iota((1, wide), 1) // MODES
    held = half_held() == 0
    half = count // 2
    tiles = []
    for k in range(count):
        line = 8 * (k % half)
        ours, theirs = mine_ref[line : line + 8, :], other_ref[line : line + 8, :]
        tiles.append(jnp.where(held, ours, theirs) if k < half else jnp.where(held, theirs, ours))

    def rows_of(start):
        sides = []
        for k in (start, start + 1):
            tile = tiles[k] * scale_ref[k]
            blocks = []
            for q in range(4):
                one = jnp.where(lane_group == q, tile, 0.0)
                one = one + pltpu.roll(one, MODES, 1)
                blocks.append(one + pltpu.roll(one, 2 * MODES, 1))
            high, low = split(jnp.concatenate(blocks, axis=0))
            sides.append(jnp.concatenate([high, low, high, jnp.zeros_like(high)], axis=0))
        both = dot(r_ref[...], jnp.concatenate(sides, axis=1))
        for i, k in enumerate((start, start + 1)):
            high, low = split(both[:, wide * i : wide * (i + 1)])
            z_ref[k] = jnp.where(lane_group == 1, low, high)

    for start in range(0, AHEAD, 2):
        rows_of(start)
    at = (iota((levels, variables), 0), iota((levels, variables), 1))
    energy = jnp.zeros((levels, variables), F32)
    for k, tile in enumerate(tiles):
        here = (at[0] == k // variables) & (at[1] == k % variables)
        energy = jnp.where(here, jnp.sum(tile * tile) / F32(MODES * MODES), energy)
    e_ref[...] = energy

    copies = [pltpu.make_async_copy(e_ref, energy_hbm, e_sem)]
    for k in range(count):
        if k % 2 == 0 and k + AHEAD < count:
            rows_of(k + AHEAD)
        o_buf[k] = (weight_ref[k // variables] * dot(z_ref[k], t_ref[...])).astype(BF16)
        copies[k].start()
        copies.append(pltpu.make_async_copy(o_buf.at[k], out_hbm.at[k], o_sem.at[k]))
    copies[-1].start()
    for copy in copies:
        copy.wait()


def in_vmem(value):
    return pltpu.with_memory_space_constraint(value, pltpu.VMEM)


def total(parts):
    while len(parts) > 1:
        parts = [a + b for a, b in zip(parts[::2], parts[1::2])]
    return parts[0]


def per_device(prognostic_values, forcing_host_values, strength, level_height, pbl_height):
    levels, variables, rows, cols = prognostic_values.shape
    nx, ny = rows * lax.axis_size("gx"), cols * lax.axis_size("gy")
    count = levels * variables
    lines = 8 * count
    wide = 4 * MODES
    anywhere = pl.BlockSpec(memory_space=pl.ANY)
    vmem = pl.BlockSpec(memory_space=pltpu.VMEM)
    smem = pl.BlockSpec(memory_space=pltpu.SMEM)

    mine, other = pl.pallas_call(
        lambda *refs: analysis(count, nx, ny, *refs),
        name="analysis",
        out_shape=(pltpu.VMEM((lines // 2, wide), F32), pltpu.VMEM((lines // 2, wide), F32)),
        in_specs=[anywhere, anywhere],
        out_specs=(vmem, vmem),
        scratch_shapes=[
            pltpu.VMEM((count, rows, cols), F32),
            pltpu.VMEM((count, rows, cols), BF16),
            pltpu.SemaphoreType.DMA((count // CHUNK,)),
            pltpu.SemaphoreType.DMA((count // CHUNK,)),
            pltpu.VMEM((cols, 2 * wide), BF16),
            pltpu.VMEM((lines, wide), F32),
        ],
    )(prognostic_values.reshape(count, rows, cols), forcing_host_values.reshape(count, rows, cols))

    prepared = pl.pallas_call(
        lambda *refs: preparation(levels, variables, nx, ny, *refs),
        name="preparation",
        out_shape=(
            pltpu.VMEM((levels, rows, cols), F32),
            pltpu.VMEM((rows, wide), BF16),
            pltpu.VMEM((wide, cols), BF16),
            pltpu.VMEM((count, 8, wide), F32),
        ),
        in_specs=[smem, smem, vmem],
        out_specs=(vmem, vmem, vmem, vmem),
    )(strength, level_height, in_vmem(pbl_height))

    held = mine + lax.ppermute(other, BOTH, CHIP)
    for at, exchange in enumerate(EXCHANGES):
        if at == len(EXCHANGES) - 1:
            held, prepared = lax.optimization_barrier((held, prepared))
        held = total([held] + [lax.ppermute(held, BOTH, pairs) for pairs in exchange])
    other = lax.ppermute(held, BOTH, CHIP)

    tendency, energy = pl.pallas_call(
        lambda *refs: synthesis(levels, variables, *refs),
        name="synthesis",
        out_shape=(
            jax.ShapeDtypeStruct((count, rows, cols), BF16),
            jax.ShapeDtypeStruct((levels, variables), F32),
        ),
        in_specs=[vmem] * 6,
        out_specs=(anywhere, anywhere),
        scratch_shapes=[
            pltpu.VMEM((count, rows, cols), BF16),
            pltpu.SemaphoreType.DMA((count,)),
            pltpu.VMEM((count, rows, wide), BF16),
            pltpu.VMEM((levels, variables), F32),
            pltpu.SemaphoreType.DMA,
        ],
    )(in_vmem(held), in_vmem(other), *map(in_vmem, prepared))
    return tendency.reshape(levels, variables, rows, cols), energy


def solution(mesh):
    return jax.shard_map(
        per_device,
        mesh=mesh,
        in_specs=(P(None, None, "gx", "gy"), P(None, None, "gx", "gy"), P(), P(), P("gx", "gy")),
        out_specs=(P(None, None, "gx", "gy"), P()),
        check_vma=False,
    )
```

```python
import math

import jax
import jax.numpy as jnp
from jax import lax
from jax.experimental import pallas as pl
from jax.experimental.pallas import tpu as pltpu
from jax.sharding import PartitionSpec as P

MODES = 32
RAMP = 0.25
BOTH = ("gx", "gy")
F32, BF16 = jnp.float32, jnp.bfloat16


def position(x, y, z, core):
    return ((z * 4 + (y // 2) * 2 + core) * 8) + (y % 2) * 4 + x


def partners(move):
    places = [(x, y, z, c) for z in range(8) for y in range(4) for x in range(4) for c in range(2)]
    return [(position(*place), position(*move(*place))) for place in places]


CHIP = partners(lambda x, y, z, c: (x, y, z, 1 - c))
EXCHANGES = (
    (
        partners(lambda x, y, z, c: (x, y, z ^ 2, 1 - c)),
        partners(lambda x, y, z, c: (x, y, z ^ 1, c)),
        partners(lambda x, y, z, c: (x, y, z ^ 3, 1 - c)),
    ),
    (partners(lambda x, y, z, c: (x, y, z ^ 7, 1 - c)),),
    (
        partners(lambda x, y, z, c: (x ^ 1, y, z, 1 - c)),
        partners(lambda x, y, z, c: (x ^ 2, y, z, c)),
        partners(lambda x, y, z, c: (x ^ 3, y, z, 1 - c)),
    ),
    (
        partners(lambda x, y, z, c: (x, y ^ 1, z, 1 - c)),
        partners(lambda x, y, z, c: (x, y ^ 2, z, c)),
        partners(lambda x, y, z, c: (x, y ^ 3, z, 1 - c)),
    ),
)


def half_held():
    gx, gy = lax.axis_index("gx"), lax.axis_index("gy")
    return (gx // 8 + gx + gy // 4 + gy) & 1


def cosines(index, wave, total):
    turn = ((2 * index + 1) * wave) & (4 * total - 1)
    turn = jnp.where(turn > 2 * total, 4 * total - turn, turn)
    y = (total - turn).astype(F32) * F32(math.pi / (2 * total))
    square = y * y
    series = F32(1.0 / math.factorial(13))
    for power in (11, 9, 7, 5, 3, 1):
        sign = -1.0 if power % 4 == 3 else 1.0
        series = series * square + F32(sign / math.factorial(power))
    scale = jnp.where(wave == 0, F32(math.sqrt(1.0 / total)), F32(math.sqrt(2.0 / total)))
    return scale * (y * series)


def split(value):
    high = value.astype(BF16)
    return high, (value - high.astype(F32)).astype(BF16)


def iota(shape, dim):
    return lax.broadcasted_iota(jnp.int32, shape, dim)


def dot(a, b):
    return jnp.dot(a, b, preferred_element_type=F32)


CHUNK = 6


def analysis(
    count, nx, ny, p_hbm, f_hbm, mine_ref, other_ref, p_buf, f_buf, p_sem, f_sem, w_ref, out_ref
):
    rows, cols = p_hbm.shape[1:]
    copies = []
    for at, start in enumerate(range(0, count, CHUNK)):
        chunk = pl.ds(start, CHUNK)
        pair = (
            pltpu.make_async_copy(p_hbm.at[chunk], p_buf.at[chunk], p_sem.at[at]),
            pltpu.make_async_copy(f_hbm.at[chunk], f_buf.at[chunk], f_sem.at[at]),
        )
        for copy in pair:
            copy.start()
        copies.append(pair)

    row0 = lax.axis_index("gx") * rows
    col0 = lax.axis_index("gy") * cols
    wide = 4 * MODES
    table = cosines(col0 + iota((cols, wide), 0), iota((cols, wide), 1) & (MODES - 1), ny)
    high, low = split(table)
    w_ref[:, :wide] = high
    w_ref[:, wide:] = low
    table = cosines(row0 + iota((MODES, rows), 1), iota((MODES, rows), 0), nx)
    high, low = split(table)
    row_table = jnp.concatenate(
        [jnp.concatenate([high, high], axis=1), jnp.concatenate([low, low], axis=1)], axis=0
    )
    lane_group = iota((8, wide), 1) // MODES

    for pair, start in zip(copies, range(0, count, CHUNK)):
        for copy in pair:
            copy.wait()
        parts = []
        for k in range(start, start + CHUNK):
            diff = jnp.concatenate(split(f_buf[k].astype(F32) - p_buf[k]), axis=0)
            both = dot(row_table, diff)
            parts.append(both[:MODES] + both[MODES:])
        part = jnp.concatenate(split(jnp.concatenate(parts, axis=0)), axis=0)
        both = dot(part, w_ref[...])
        both = both[: CHUNK * MODES] + both[CHUNK * MODES :]
        both = both[:, :wide] + both[:, wide:]
        for i in range(CHUNK):
            coefs = both[MODES * i : MODES * (i + 1)]
            tile = coefs[:8]
            for q in range(1, 4):
                tile = jnp.where(lane_group == q, coefs[8 * q : 8 * q + 8], tile)
            line = 8 * (start + i)
            out_ref[line : line + 8, :] = tile
    half = out_ref.shape[0] // 2
    first, second = out_ref[:half, :], out_ref[half:, :]
    held = half_held() == 0
    mine_ref[...] = jnp.where(held, first, second)
    other_ref[...] = jnp.where(held, second, first)


def preparation(
    levels, variables, nx, ny, strength_ref, level_ref, pbl_ref, weight_ref, r_ref, t_ref, scale_ref
):
    rows, cols = pbl_ref.shape
    row0 = lax.axis_index("gx") * rows
    col0 = lax.axis_index("gy") * cols
    wide = 4 * MODES
    for l in range(levels):
        weight_ref[l] = 1.0 / (1.0 + jnp.exp(-(level_ref[l] - pbl_ref[...]) / F32(RAMP)))
        for v in range(variables):
            scale_ref[l * variables + v] = jnp.full((8, wide), strength_ref[l, v], F32)
    lane_group = iota((1, wide), 1) // MODES
    high, low = split(cosines(row0 + iota((rows, wide), 0), iota((rows, wide), 1) & (MODES - 1), nx))
    none = jnp.zeros_like(high)
    r_ref[...] = jnp.where(lane_group < 2, high, jnp.where(lane_group == 2, low, none))
    high, low = split(cosines(col0 + iota((MODES, cols), 1), iota((MODES, cols), 0), ny))
    t_ref[0:32, :] = high
    t_ref[32:64, :] = high
    t_ref[64:96, :] = low
    t_ref[96:128, :] = jnp.zeros_like(high)


AHEAD = 6


def synthesis(
    levels, variables,
    mine_ref, other_ref, weight_ref, r_ref, t_ref, scale_ref,
    out_hbm, energy_hbm, o_buf, o_sem, z_ref, e_ref, e_sem,
):
    count = levels * variables
    wide = 4 * MODES
    lane_group = iota((1, wide), 1) // MODES
    held = half_held() == 0
    half = count // 2
    tiles = []
    for k in range(count):
        line = 8 * (k % half)
        ours, theirs = mine_ref[line : line + 8, :], other_ref[line : line + 8, :]
        tiles.append(jnp.where(held, ours, theirs) if k < half else jnp.where(held, theirs, ours))

    def rows_of(start):
        sides = []
        for k in (start, start + 1):
            tile = tiles[k] * scale_ref[k]
            blocks = []
            for q in range(4):
                one = jnp.where(lane_group == q, tile, 0.0)
                one = one + pltpu.roll(one, MODES, 1)
                blocks.append(one + pltpu.roll(one, 2 * MODES, 1))
            high, low = split(jnp.concatenate(blocks, axis=0))
            sides.append(jnp.concatenate([high, low, high, jnp.zeros_like(high)], axis=0))
        both = dot(r_ref[...], jnp.concatenate(sides, axis=1))
        for i, k in enumerate((start, start + 1)):
            high, low = split(both[:, wide * i : wide * (i + 1)])
            z_ref[k] = jnp.where(lane_group == 1, low, high)

    for start in range(0, AHEAD, 2):
        rows_of(start)
    at = (iota((levels, variables), 0), iota((levels, variables), 1))
    energy = jnp.zeros((levels, variables), F32)
    for k, tile in enumerate(tiles):
        here = (at[0] == k // variables) & (at[1] == k % variables)
        energy = jnp.where(here, jnp.sum(tile * tile) / F32(MODES * MODES), energy)
    e_ref[...] = energy

    copies = [pltpu.make_async_copy(e_ref, energy_hbm, e_sem)]
    for k in range(count):
        if k % 2 == 0 and k + AHEAD < count:
            rows_of(k + AHEAD)
        o_buf[k] = (weight_ref[k // variables] * dot(z_ref[k], t_ref[...])).astype(BF16)
        copies[k].start()
        copies.append(pltpu.make_async_copy(o_buf.at[k], out_hbm.at[k], o_sem.at[k]))
    copies[-1].start()
    for copy in copies:
        copy.wait()


def in_vmem(value):
    return pltpu.with_memory_space_constraint(value, pltpu.VMEM)


def total(parts):
    while len(parts) > 1:
        parts = [a + b for a, b in zip(parts[::2], parts[1::2])]
    return parts[0]


def per_device(prognostic_values, forcing_host_values, strength, level_height, pbl_height):
    levels, variables, rows, cols = prognostic_values.shape
    nx, ny = rows * lax.axis_size("gx"), cols * lax.axis_size("gy")
    count = levels * variables
    lines = 8 * count
    wide = 4 * MODES
    anywhere = pl.BlockSpec(memory_space=pl.ANY)
    vmem = pl.BlockSpec(memory_space=pltpu.VMEM)
    smem = pl.BlockSpec(memory_space=pltpu.SMEM)

    mine, other = pl.pallas_call(
        lambda *refs: analysis(count, nx, ny, *refs),
        name="analysis",
        out_shape=(pltpu.VMEM((lines // 2, wide), F32), pltpu.VMEM((lines // 2, wide), F32)),
        in_specs=[anywhere, anywhere],
        out_specs=(vmem, vmem),
        scratch_shapes=[
            pltpu.VMEM((count, rows, cols), F32),
            pltpu.VMEM((count, rows, cols), BF16),
            pltpu.SemaphoreType.DMA((count // CHUNK,)),
            pltpu.SemaphoreType.DMA((count // CHUNK,)),
            pltpu.VMEM((cols, 2 * wide), BF16),
            pltpu.VMEM((lines, wide), F32),
        ],
    )(prognostic_values.reshape(count, rows, cols), forcing_host_values.reshape(count, rows, cols))

    prepared = pl.pallas_call(
        lambda *refs: preparation(levels, variables, nx, ny, *refs),
        name="preparation",
        out_shape=(
            pltpu.VMEM((levels, rows, cols), F32),
            pltpu.VMEM((rows, wide), BF16),
            pltpu.VMEM((wide, cols), BF16),
            pltpu.VMEM((count, 8, wide), F32),
        ),
        in_specs=[smem, smem, vmem],
        out_specs=(vmem, vmem, vmem, vmem),
    )(strength, level_height, in_vmem(pbl_height))

    held = mine + lax.ppermute(other, BOTH, CHIP)
    for at, exchange in enumerate(EXCHANGES):
        if at == 2:
            held, prepared = lax.optimization_barrier((held, prepared))
        held = total([held] + [lax.ppermute(held, BOTH, pairs) for pairs in exchange])
    other = lax.ppermute(held, BOTH, CHIP)

    tendency, energy = pl.pallas_call(
        lambda *refs: synthesis(levels, variables, *refs),
        name="synthesis",
        out_shape=(
            jax.ShapeDtypeStruct((count, rows, cols), BF16),
            jax.ShapeDtypeStruct((levels, variables), F32),
        ),
        in_specs=[vmem] * 6,
        out_specs=(anywhere, anywhere),
        scratch_shapes=[
            pltpu.VMEM((count, rows, cols), BF16),
            pltpu.SemaphoreType.DMA((count,)),
            pltpu.VMEM((count, rows, wide), BF16),
            pltpu.VMEM((levels, variables), F32),
            pltpu.SemaphoreType.DMA,
        ],
    )(in_vmem(held), in_vmem(other), *map(in_vmem, prepared))
    return tendency.reshape(levels, variables, rows, cols), energy


def solution(mesh):
    return jax.shard_map(
        per_device,
        mesh=mesh,
        in_specs=(P(None, None, "gx", "gy"), P(None, None, "gx", "gy"), P(), P(), P("gx", "gy")),
        out_specs=(P(None, None, "gx", "gy"), P()),
        check_vma=False,
    )
```

```python
import math

import jax
import jax.numpy as jnp
from jax import lax
from jax.experimental import pallas as pl
from jax.experimental.pallas import tpu as pltpu
from jax.sharding import PartitionSpec as P

MODES = 32
RAMP = 0.25
BOTH = ("gx", "gy")
F32, BF16 = jnp.float32, jnp.bfloat16


def position(x, y, z, core):
    return ((z * 4 + (y // 2) * 2 + core) * 8) + (y % 2) * 4 + x


def partners(move):
    places = [(x, y, z, c) for z in range(8) for y in range(4) for x in range(4) for c in range(2)]
    return [(position(*place), position(*move(*place))) for place in places]


CHIP = partners(lambda x, y, z, c: (x, y, z, 1 - c))
EXCHANGES = (
    (
        partners(lambda x, y, z, c: (x, y, z ^ 2, 1 - c)),
        partners(lambda x, y, z, c: (x, y, z ^ 1, c)),
        partners(lambda x, y, z, c: (x, y, z ^ 3, 1 - c)),
    ),
    (partners(lambda x, y, z, c: (x, y, z ^ 7, 1 - c)),),
    (
        partners(lambda x, y, z, c: (x ^ 1, y, z, 1 - c)),
        partners(lambda x, y, z, c: (x ^ 2, y, z, c)),
        partners(lambda x, y, z, c: (x ^ 3, y, z, 1 - c)),
    ),
    (
        partners(lambda x, y, z, c: (x, y ^ 1, z, 1 - c)),
        partners(lambda x, y, z, c: (x, y ^ 2, z, c)),
        partners(lambda x, y, z, c: (x, y ^ 3, z, 1 - c)),
    ),
)


def half_held():
    gx, gy = lax.axis_index("gx"), lax.axis_index("gy")
    return (gx // 8 + gx + gy // 4 + gy) & 1


def cosines(index, wave, total):
    turn = ((2 * index + 1) * wave) & (4 * total - 1)
    turn = jnp.where(turn > 2 * total, 4 * total - turn, turn)
    y = (total - turn).astype(F32) * F32(math.pi / (2 * total))
    square = y * y
    series = F32(1.0 / math.factorial(13))
    for power in (11, 9, 7, 5, 3, 1):
        sign = -1.0 if power % 4 == 3 else 1.0
        series = series * square + F32(sign / math.factorial(power))
    scale = jnp.where(wave == 0, F32(math.sqrt(1.0 / total)), F32(math.sqrt(2.0 / total)))
    return scale * (y * series)


def split(value):
    high = value.astype(BF16)
    return high, (value - high.astype(F32)).astype(BF16)


def iota(shape, dim):
    return lax.broadcasted_iota(jnp.int32, shape, dim)


def dot(a, b):
    return jnp.dot(a, b, preferred_element_type=F32)


CHUNKS = (5, 4)


def transformed(p_buf, f_buf, start, size, row_table, w, out_ref):
    wide = 4 * MODES
    lane_group = iota((8, wide), 1) // MODES
    parts = []
    for k in range(start, start + size):
        diff = jnp.concatenate(split(f_buf[k].astype(F32) - p_buf[k]), axis=0)
        both = dot(row_table, diff)
        parts.append(both[:MODES] + both[MODES:])
    part = jnp.concatenate(split(jnp.concatenate(parts, axis=0)), axis=0)
    both = dot(part, w)
    both = both[: size * MODES] + both[size * MODES :]
    both = both[:, :wide] + both[:, wide:]
    for i in range(size):
        coefs = both[MODES * i : MODES * (i + 1)]
        tile = coefs[:8]
        for q in range(1, 4):
            tile = jnp.where(lane_group == q, coefs[8 * q : 8 * q + 8], tile)
        out_ref[8 * (start + i) : 8 * (start + i) + 8, :] = tile


def analysis_other(
    count, nx, ny, p_hbm, f_hbm, other_ref, p_mine, f_mine, w_ref, r_ref, p_buf, f_buf, p_sem, f_sem
):
    rows, cols = p_hbm.shape[1:]
    half = count // 2
    mine = half_held() * half
    copies = []
    for at, size in enumerate(CHUNKS):
        there, here = pl.ds(half - mine + sum(CHUNKS[:at]), size), pl.ds(sum(CHUNKS[:at]), size)
        copies.append((
            pltpu.make_async_copy(p_hbm.at[there], p_buf.at[here], p_sem.at[at]),
            pltpu.make_async_copy(f_hbm.at[there], f_buf.at[here], f_sem.at[at]),
        ))
    copies.append((
        pltpu.make_async_copy(p_hbm.at[pl.ds(mine, half)], p_mine, p_sem.at[len(CHUNKS)]),
        pltpu.make_async_copy(f_hbm.at[pl.ds(mine, half)], f_mine, f_sem.at[len(CHUNKS)]),
    ))
    for pair in copies:
        for copy in pair:
            copy.start()

    row0 = lax.axis_index("gx") * rows
    col0 = lax.axis_index("gy") * cols
    wide = 4 * MODES
    table = cosines(col0 + iota((cols, wide), 0), iota((cols, wide), 1) & (MODES - 1), ny)
    high, low = split(table)
    w_ref[:, :wide] = high
    w_ref[:, wide:] = low
    table = cosines(row0 + iota((MODES, rows), 1), iota((MODES, rows), 0), nx)
    high, low = split(table)
    row_table = jnp.concatenate(
        [jnp.concatenate([high, high], axis=1), jnp.concatenate([low, low], axis=1)], axis=0
    )
    r_ref[...] = row_table
    for at, size in enumerate(CHUNKS):
        for copy in copies[at]:
            copy.wait()
        transformed(p_buf, f_buf, sum(CHUNKS[:at]), size, row_table, w_ref[...], other_ref)
    for copy in copies[-1]:
        copy.wait()


def analysis_mine(count, p_ref, f_ref, w_ref, r_ref, mine_ref):
    transformed(p_ref, f_ref, 0, count // 2, r_ref[...], w_ref[...], mine_ref)


def preparation(
    levels, variables, nx, ny, strength_ref, level_ref, pbl_ref, weight_ref, r_ref, t_ref, scale_ref
):
    rows, cols = pbl_ref.shape
    row0 = lax.axis_index("gx") * rows
    col0 = lax.axis_index("gy") * cols
    wide = 4 * MODES
    for l in range(levels):
        weight_ref[l] = 1.0 / (1.0 + jnp.exp(-(level_ref[l] - pbl_ref[...]) / F32(RAMP)))
        for v in range(variables):
            scale_ref[l * variables + v] = jnp.full((8, wide), strength_ref[l, v], F32)
    lane_group = iota((1, wide), 1) // MODES
    high, low = split(cosines(row0 + iota((rows, wide), 0), iota((rows, wide), 1) & (MODES - 1), nx))
    none = jnp.zeros_like(high)
    r_ref[...] = jnp.where(lane_group < 2, high, jnp.where(lane_group == 2, low, none))
    high, low = split(cosines(col0 + iota((MODES, cols), 1), iota((MODES, cols), 0), ny))
    t_ref[0:32, :] = high
    t_ref[32:64, :] = high
    t_ref[64:96, :] = low
    t_ref[96:128, :] = jnp.zeros_like(high)


AHEAD = 6


def synthesis(
    levels, variables,
    mine_ref, other_ref, weight_ref, r_ref, t_ref, scale_ref,
    out_hbm, energy_hbm, o_buf, o_sem, z_ref, e_ref, e_sem,
):
    count = levels * variables
    wide = 4 * MODES
    lane_group = iota((1, wide), 1) // MODES
    held = half_held() == 0
    half = count // 2
    tiles = []
    for k in range(count):
        line = 8 * (k % half)
        ours, theirs = mine_ref[line : line + 8, :], other_ref[line : line + 8, :]
        tiles.append(jnp.where(held, ours, theirs) if k < half else jnp.where(held, theirs, ours))

    def rows_of(start):
        sides = []
        for k in (start, start + 1):
            tile = tiles[k] * scale_ref[k]
            blocks = []
            for q in range(4):
                one = jnp.where(lane_group == q, tile, 0.0)
                one = one + pltpu.roll(one, MODES, 1)
                blocks.append(one + pltpu.roll(one, 2 * MODES, 1))
            high, low = split(jnp.concatenate(blocks, axis=0))
            sides.append(jnp.concatenate([high, low, high, jnp.zeros_like(high)], axis=0))
        both = dot(r_ref[...], jnp.concatenate(sides, axis=1))
        for i, k in enumerate((start, start + 1)):
            high, low = split(both[:, wide * i : wide * (i + 1)])
            z_ref[k] = jnp.where(lane_group == 1, low, high)

    for start in range(0, AHEAD, 2):
        rows_of(start)
    at = (iota((levels, variables), 0), iota((levels, variables), 1))
    energy = jnp.zeros((levels, variables), F32)
    for k, tile in enumerate(tiles):
        here = (at[0] == k // variables) & (at[1] == k % variables)
        energy = jnp.where(here, jnp.sum(tile * tile) / F32(MODES * MODES), energy)
    e_ref[...] = energy

    copies = [pltpu.make_async_copy(e_ref, energy_hbm, e_sem)]
    for k in range(count):
        if k % 2 == 0 and k + AHEAD < count:
            rows_of(k + AHEAD)
        o_buf[k] = (weight_ref[k // variables] * dot(z_ref[k], t_ref[...])).astype(BF16)
        copies[k].start()
        copies.append(pltpu.make_async_copy(o_buf.at[k], out_hbm.at[k], o_sem.at[k]))
    copies[-1].start()
    for copy in copies:
        copy.wait()


def in_hbm(value):
    return pltpu.with_memory_space_constraint(value, pltpu.HBM)


def in_vmem(value):
    return pltpu.with_memory_space_constraint(value, pltpu.VMEM)


def total(parts):
    while len(parts) > 1:
        parts = [a + b for a, b in zip(parts[::2], parts[1::2])]
    return parts[0]


def per_device(prognostic_values, forcing_host_values, strength, level_height, pbl_height):
    levels, variables, rows, cols = prognostic_values.shape
    nx, ny = rows * lax.axis_size("gx"), cols * lax.axis_size("gy")
    count = levels * variables
    lines = 8 * count
    wide = 4 * MODES
    anywhere = pl.BlockSpec(memory_space=pl.ANY)
    vmem = pl.BlockSpec(memory_space=pltpu.VMEM)
    smem = pl.BlockSpec(memory_space=pltpu.SMEM)

    half = count // 2
    other, *kept = pl.pallas_call(
        lambda *refs: analysis_other(count, nx, ny, *refs),
        name="analysis_other",
        out_shape=(
            pltpu.VMEM((lines // 2, wide), F32),
            pltpu.VMEM((half, rows, cols), F32),
            pltpu.VMEM((half, rows, cols), BF16),
            pltpu.VMEM((cols, 2 * wide), BF16),
            pltpu.VMEM((2 * MODES, 2 * rows), BF16),
        ),
        in_specs=[anywhere, anywhere],
        out_specs=(vmem,) * 5,
        compiler_params=pltpu.CompilerParams(vmem_limit_bytes=24 << 20),
        scratch_shapes=[
            pltpu.VMEM((half, rows, cols), F32),
            pltpu.VMEM((half, rows, cols), BF16),
            pltpu.SemaphoreType.DMA((len(CHUNKS) + 1,)),
            pltpu.SemaphoreType.DMA((len(CHUNKS) + 1,)),
        ],
    )(
        in_hbm(prognostic_values.reshape(count, rows, cols)),
        in_hbm(forcing_host_values.reshape(count, rows, cols)),
    )
    arriving = lax.ppermute(other, BOTH, CHIP)
    mine = pl.pallas_call(
        lambda *refs: analysis_mine(count, *refs),
        name="analysis_mine",
        out_shape=pltpu.VMEM((lines // 2, wide), F32),
        in_specs=[vmem] * 4,
        out_specs=vmem,
        compiler_params=pltpu.CompilerParams(vmem_limit_bytes=24 << 20),
    )(*map(in_vmem, kept))

    prepared = pl.pallas_call(
        lambda *refs: preparation(levels, variables, nx, ny, *refs),
        name="preparation",
        out_shape=(
            pltpu.VMEM((levels, rows, cols), F32),
            pltpu.VMEM((rows, wide), BF16),
            pltpu.VMEM((wide, cols), BF16),
            pltpu.VMEM((count, 8, wide), F32),
        ),
        in_specs=[smem, smem, vmem],
        out_specs=(vmem, vmem, vmem, vmem),
    )(strength, level_height, in_vmem(pbl_height))

    held = mine + arriving
    for at, exchange in enumerate(EXCHANGES):
        if at == 2:
            held, prepared = lax.optimization_barrier((held, prepared))
        arrived = [lax.ppermute(held, BOTH, pairs) for pairs in reversed(exchange)]
        held = total([held] + arrived)
    other = lax.ppermute(held, BOTH, CHIP)

    tendency, energy = pl.pallas_call(
        lambda *refs: synthesis(levels, variables, *refs),
        name="synthesis",
        out_shape=(
            jax.ShapeDtypeStruct((count, rows, cols), BF16),
            jax.ShapeDtypeStruct((levels, variables), F32),
        ),
        in_specs=[vmem] * 6,
        out_specs=(anywhere, anywhere),
        scratch_shapes=[
            pltpu.VMEM((count, rows, cols), BF16),
            pltpu.SemaphoreType.DMA((count,)),
            pltpu.VMEM((count, rows, wide), BF16),
            pltpu.VMEM((levels, variables), F32),
            pltpu.SemaphoreType.DMA,
        ],
    )(in_vmem(held), in_vmem(other), *map(in_vmem, prepared))
    return tendency.reshape(levels, variables, rows, cols), energy


def solution(mesh):
    return jax.shard_map(
        per_device,
        mesh=mesh,
        in_specs=(P(None, None, "gx", "gy"), P(None, None, "gx", "gy"), P(), P(), P("gx", "gy")),
        out_specs=(P(None, None, "gx", "gy"), P()),
        check_vma=False,
    )
```
